32 devices in a mesh: env: 4 (over z), tm: 8 (over y, x, core).
Axes of the slice: x: 2, y: 2, z: 4, core: 2. Of those that a mesh axis runs over, the one named last changes fastest.
Arguments:
- observations: bfloat16 [8, 6144, 2048], P('env', 'tm'), may hold values from -6 to 6
- stored_values: float32 [8, 6144], P('env', 'tm'), may hold values from -3.6 to 3.6
- rewards: float32 [8, 6144], P('env', 'tm'), may hold values from -0.18 to 0.18
- episode_ends: int32 [8, 6144], P('env', 'tm'), may hold values 0 or 1
- stale_list: int32 [4, 8, 12], P('env', 'tm'), may hold values from -1 to 11, as said below
- discount_horizon: float32 [8], P('env'), may hold values from 10 to 49152
- trace_horizon: float32 [8], P('env'), may hold values from 10 to 49152
- bootstrap: float32 [8], P('env'), may hold values from -3.6 to 3.6
- norm_gain: float32 [2048], replicated, may hold values from 0.1 to 1.9
- input_weight: bfloat16 [2048, 4096], replicated, may hold values from -0.125 to 0.125
- value_head: bfloat16 [4096], replicated, may hold values from -0.09375 to 0.09375
Outputs:
- targets: float32 [8, 6144], P('env', 'tm')
- advantages: float32 [8, 6144], P('env', 'tm')
The draws below stay inside these ranges and needn't reach their ends.
Inputs may be any that keep to these rules, and one draw needn't show every extreme that they name: `stale_list`: for each device (first two indices: env shard, time shard) the last dimension lists distinct local block numbers e * 6 + k (e an environment row within the env shard, k a block of 128 steps within the time shard), followed by -1 entries; on some device all 12 blocks are listed.
All inputs are finite; a program needn't handle non-finite values. No bound on the sum of `episode_ends` on one device may be relied on, other than what follows from the above.
Results may differ from the reference program's by a relative error of at most 0.0018.
Values may be sent and summed in bfloat16 or wider, within the bound.
A program may use at most 128 MiB of HBM per device.

```python
import jax
import jax.numpy as jnp
from jax import lax

D = 2048
FF = 4096
BLOCK = 128
ENV_DEV = 2
NB = 6
BLK_DEV = 12
SEQ = 6144
B = 8
N_ENV = 4
N_TM = 8


def draw_stale_list(key, part):
    device_count = N_ENV * N_TM
    device_keys = jax.random.split(jax.random.fold_in(key, 11), device_count)
    shuffled = jax.vmap(lambda one_key: jax.random.permutation(one_key, BLK_DEV))(device_keys)
    first_count = jax.random.randint(jax.random.fold_in(key, 12), (device_count,), 0, BLK_DEV + 1)
    second_count = jax.random.randint(jax.random.fold_in(key, 13), (device_count,), 0, BLK_DEV + 1)
    counts = jnp.minimum(first_count, second_count)
    busiest = jax.random.randint(jax.random.fold_in(key, 14), (), 0, device_count)
    counts = jnp.where(jnp.arange(device_count) == busiest, BLK_DEV, counts)
    listed = jnp.where(jnp.arange(BLK_DEV)[None, :] < counts[:, None], shuffled, -1)
    return listed.reshape(N_ENV, N_TM, BLK_DEV).astype(jnp.int32)


def draw_rewards(key, part):
    env_position = jnp.arange(B, dtype=jnp.float32) / max(B - 1, 1)
    scales = 0.005 * 9.0 ** env_position
    draw_noise = jnp.clip(jax.random.normal(jax.random.fold_in(key, 32), (B, SEQ), jnp.float32), -4.0, 4.0)
    return (draw_noise * scales[:, None]).astype(jnp.float32)


def horizon_draw(key, salt):
    slow_share = 0.5
    is_slow = jax.random.bernoulli(jax.random.fold_in(key, 21), slow_share, (B,))
    level = jax.random.uniform(jax.random.fold_in(key, salt), (B,), jnp.float32, 0.0, 1.0)
    fast_value = 10.0 * 4.0 ** level
    slow_value = 2.0 * SEQ * 4.0 ** level
    return jnp.where(is_slow, slow_value, fast_value).astype(jnp.float32)


def draw_discount_horizon(key, part):
    return horizon_draw(key, 22)


def draw_trace_horizon(key, part):
    return horizon_draw(key, 23)


def set_ends(values, own_key, low, largest):
    longest = values.shape.index(max(values.shape))
    spots = []
    for shift in (0, 1):
        where = [jax.random.randint(jax.random.fold_in(own_key, axis), (), 0, length) for axis, length in enumerate(values.shape)]
        where[longest] = (where[longest] + shift) % values.shape[longest]
        spots.append(tuple(where))
    return values.at[spots[0]].set(low).at[spots[1]].set(largest)


def levels(rng, shape, pieces, least, high):
    factor_of = 1.0
    for dim, parts in pieces:
        heights = jax.random.uniform(jax.random.fold_in(jax.random.fold_in(rng, 6), dim), (parts,), jnp.float32, least / len(pieces), high / len(pieces))
        factor_of = factor_of * jnp.repeat(jnp.exp(heights), shape[dim] // parts).reshape((-1,) + (1,) * (len(shape) - 1 - dim))
    return factor_of


def scatter_about(rng, extent, deviation, most, cuts=(), kind=jnp.bfloat16):
    loudness = levels(rng, extent, cuts, -0.22, 0.18) if cuts else 1.0
    values = jax.random.normal(rng, extent, jnp.float32) * deviation * loudness
    return jnp.minimum(jnp.maximum(values, -most), most).astype(kind)


def setup_inputs(seed: int = 0) -> dict:
    streams_of = jax.random.split(jax.random.key(seed), 12)
    observations = scatter_about(streams_of[0], (B, SEQ, D), 1.0, 6.0, ((0, 4), (1, 8)))
    stored_values = scatter_about(streams_of[1], (B, SEQ), 0.6, 3.6, ((0, 4), (1, 8)), jnp.float32)
    rewards = draw_rewards(jax.random.fold_in(streams_of[11], 71), 0)
    episode_ends = set_ends((jax.random.randint(streams_of[3], (B, SEQ), 0, SEQ // 2) < 1).astype(jnp.int32), jax.random.fold_in(streams_of[3], 1), 0, 1)
    stale_list = draw_stale_list(jax.random.fold_in(streams_of[11], 71), 0)
    discount_horizon = draw_discount_horizon(jax.random.fold_in(streams_of[11], 71), 0)
    trace_horizon = draw_trace_horizon(jax.random.fold_in(streams_of[11], 71), 0)
    bootstrap = scatter_about(streams_of[7], (B,), 0.6, 3.6, ((0, 4),), jnp.float32)
    norm_gain = jnp.clip(1.0 + 0.18 * jax.random.normal(streams_of[8], (D,), jnp.float32), 0.1, 1.9)
    input_weight = scatter_about(streams_of[9], (D, FF), D ** -0.5, 0.125)
    value_head = scatter_about(streams_of[10], (FF,), FF ** -0.5, 0.09375)
    return {"observations": observations, "stored_values": stored_values, "rewards": rewards, "episode_ends": episode_ends, "stale_list": stale_list, "discount_horizon": discount_horizon, "trace_horizon": trace_horizon, "bootstrap": bootstrap, "norm_gain": norm_gain, "input_weight": input_weight, "value_head": value_head}


def critic_rows(block_rows, norm_gain, input_weight, value_head):
    widened = block_rows.astype(jnp.float32)
    square_mean = lax.optimization_barrier(jnp.mean(widened * widened, axis=-1, keepdims=True))
    normed = (widened * lax.rsqrt(square_mean + 1e-05) * norm_gain).astype(jnp.bfloat16)
    hidden = jnp.dot(normed, input_weight, preferred_element_type=jnp.float32)
    active = jax.nn.silu(hidden).astype(jnp.bfloat16)
    return jnp.dot(active, value_head, preferred_element_type=jnp.float32)

def reference(observations, stored_values, rewards, episode_ends, stale_list, discount_horizon, trace_horizon, bootstrap, norm_gain, input_weight, value_head):
    env_total = ENV_DEV * N_ENV
    block_ids = jnp.arange(ENV_DEV * NB, dtype=jnp.int32)
    listed = jnp.any(stale_list[..., :, None] == block_ids[None, None, None, :], axis=-2)
    stale_blocks = listed.reshape(N_ENV, N_TM, ENV_DEV, NB).transpose(0, 2, 1, 3).reshape(env_total, N_TM * NB)
    grouped = observations.reshape(env_total * N_TM * NB, BLOCK, D)
    stale_flags = stale_blocks.reshape(-1)

    def refresh(element):
        block_rows, is_stale = element
        return lax.cond(is_stale, lambda rows_in: critic_rows(rows_in, norm_gain, input_weight, value_head), lambda rows_in: jnp.zeros((BLOCK,), jnp.float32), block_rows)
    fresh = lax.map(refresh, (grouped, stale_flags)).reshape(env_total, SEQ)
    stale_mask = jnp.repeat(stale_blocks, BLOCK, axis=1)
    values = jnp.where(stale_mask, fresh, stored_values)
    next_values = jnp.concatenate([values[:, 1:], bootstrap[:, None]], axis=1)
    discount = 1.0 - 1.0 / discount_horizon
    trace_rate = 1.0 - 1.0 / trace_horizon
    continuing = 1.0 - episode_ends.astype(jnp.float32)
    td_error = rewards + discount[:, None] * continuing * next_values - values
    decay_rate = discount[:, None] * trace_rate[:, None] * continuing

    def backward(running, element):
        error_now, decay_now = element
        updated = error_now + decay_now * running
        return (updated, updated)
    start = jnp.zeros((env_total,), jnp.float32)
    unused, adv_steps = lax.scan(backward, start, (td_error.T, decay_rate.T), reverse=True)
    adv = adv_steps.T
    targets = adv + values
    adv_mean = jnp.mean(adv)
    centered = adv - adv_mean
    adv_var = jnp.mean(centered * centered)
    advantages = centered / jnp.sqrt(adv_var + 1e-05)
    return (targets, advantages)
```

```python
import functools

import jax
import jax.numpy as jnp
from jax import lax
from jax.experimental import pallas as pl
from jax.experimental.pallas import tpu as pltpu
from jax.sharding import PartitionSpec as P

BLOCK = 128
CHUNK = 256
MESH = pl.DeviceIdType.MESH


def critic_kernel(
    list_ref, blocks_ref, weight_ref, stored_ref, gain_ref, head_ref, out_ref,
    rows_ref, w_ref, acc_ref, row_sems, w_sems,
):
    slots, steps, features = blocks_ref.shape
    env_rows = stored_ref.shape[0]
    per_env = slots // env_rows
    chunks = w_ref.shape[0]
    count = jnp.int32(0)
    for i in range(slots):
        count = count + jnp.where(list_ref[i] >= 0, 1, 0).astype(jnp.int32)

    def row_copy(i):
        number = jnp.maximum(list_ref[i], 0)
        return pltpu.make_async_copy(
            blocks_ref.at[number], rows_ref.at[pl.ds(i * steps, steps)], row_sems.at[i]
        )

    def weight_copy(c):
        return pltpu.make_async_copy(
            weight_ref.at[:, pl.ds(pl.multiple_of(c * CHUNK, CHUNK), CHUNK)], w_ref.at[c], w_sems.at[c]
        )

    for k in range(per_env):
        out_ref[k * env_rows:(k + 1) * env_rows, :] = stored_ref[:, k * steps:(k + 1) * steps]

    @pl.when(count > 0)
    def _():
        @pl.loop(0, count)
        def _(i):
            row_copy(i).start()

        @pl.loop(0, chunks)
        def _(c):
            weight_copy(c).start()

        acc_ref[...] = jnp.zeros_like(acc_ref)

        @pl.loop(0, count)
        def _(i):
            row_copy(i).wait()
            here = pl.ds(pl.multiple_of(i * steps, steps), steps)
            wide = rows_ref[here, :].astype(jnp.float32)
            mean = jnp.sum(wide * wide, axis=-1, keepdims=True) * (1.0 / features)
            rows_ref[here, :] = (wide * lax.rsqrt(mean + 1e-05) * gain_ref[...]).astype(jnp.bfloat16)

        def tile(c, start, size):
            here = pl.ds(pl.multiple_of(start, steps), size)
            hidden = jnp.dot(rows_ref[here, :], w_ref[c], preferred_element_type=jnp.float32)
            half = 0.5 * hidden
            active = (half + half * jnp.tanh(half)).astype(jnp.bfloat16).astype(jnp.float32)
            part = active * head_ref[c]
            total = part[:, :128]
            for j in range(1, CHUNK // 128):
                total = total + part[:, j * 128:(j + 1) * 128]
            acc_ref[here, :] += total

        @pl.loop(0, chunks)
        def _(c):
            weight_copy(c).wait()

            @pl.loop(0, count // 4)
            def _(q):
                tile(c, q * (4 * steps), 4 * steps)

            @pl.when(count % 4 >= 2)
            def _():
                tile(c, (count // 4) * (4 * steps), 2 * steps)

            @pl.when(count % 2 == 1)
            def _():
                tile(c, (count - 1) * steps, steps)

        @pl.loop(0, count)
        def _(i):
            here = pl.ds(pl.multiple_of(i * steps, steps), steps)
            score = jnp.sum(acc_ref[here, :].T, axis=0, keepdims=True)
            number = list_ref[i]
            out_ref[pl.ds((number % per_env) * env_rows + number // per_env, 1), :] = score


def critic_values(listed, blocks, weight, stored, gain, head):
    slots, steps, features = blocks.shape
    hidden = weight.shape[1]
    chunks = hidden // CHUNK
    vmem = pl.BlockSpec(memory_space=pltpu.VMEM)
    hbm = pl.BlockSpec(memory_space=pl.ANY)
    return pl.pallas_call(
        critic_kernel,
        out_shape=jax.ShapeDtypeStruct((slots, steps), jnp.float32),
        in_specs=[pl.BlockSpec(memory_space=pltpu.SMEM), hbm, hbm, vmem, vmem, vmem],
        out_specs=vmem,
        scratch_shapes=[
            pltpu.VMEM((slots * steps, features), jnp.bfloat16),
            pltpu.VMEM((chunks, features, CHUNK), jnp.bfloat16),
            pltpu.VMEM((slots * steps, 128), jnp.float32),
            pltpu.SemaphoreType.DMA((slots,)),
            pltpu.SemaphoreType.DMA((chunks,)),
        ],
        compiler_params=pltpu.CompilerParams(vmem_limit_bytes=60 * 1024 * 1024),
        name="critic",
    )(listed, blocks, weight, stored, gain, head)


def sweep_kernel(
    n_env, n_tm, dh_ref, th_ref, boot_ref, values_ref, rewards_ref, ends_ref, targets_ref, adv_ref,
    tm_buf, env_buf, tm_send, tm_recv, env_send, env_recv,
):
    env_rows, local_steps = rewards_ref.shape
    rows, steps = values_ref.shape
    per_env = rows // env_rows
    my_env, my_tm = lax.axis_index("env"), lax.axis_index("tm")

    barrier = pltpu.get_barrier_semaphore()
    for d in range(1, n_tm):
        pl.semaphore_signal(barrier, inc=1, device_id=(my_env, lax.rem(my_tm + d, n_tm)), device_id_type=MESH)
    for d in range(1, n_env):
        pl.semaphore_signal(barrier, inc=1, device_id=(lax.rem(my_env + d, n_env), my_tm), device_id_type=MESH)

    def stacked(ref):
        return jnp.concatenate([ref[:, k * steps:(k + 1) * steps] for k in range(per_env)], axis=0)

    def by_env(ref, shape, modulus):
        env_of = lax.broadcasted_iota(jnp.int32, shape, 0) % modulus
        out = jnp.full(shape, ref[0], jnp.float32)
        for e in range(1, env_rows):
            out = jnp.where(env_of == e, ref[e], out)
        return out

    def over_blocks(x):
        total = x[:env_rows]
        for k in range(1, per_env):
            total = total + x[k * env_rows:(k + 1) * env_rows]
        return total

    def mean_of(x):
        total = jnp.sum(over_blocks(x), axis=1, keepdims=True) * (1.0 / local_steps)
        return jnp.broadcast_to(total, (env_rows, steps))

    full = (rows, steps)
    lane = lax.broadcasted_iota(jnp.int32, full, 1)
    row = lax.broadcasted_iota(jnp.int32, full, 0)
    values = values_ref[...]
    rewards = stacked(rewards_ref)
    going = 1.0 - stacked(ends_ref).astype(jnp.float32)
    discount = 1.0 - 1.0 / by_env(dh_ref, full, env_rows)
    trace_rate = 1.0 - 1.0 / by_env(th_ref, full, env_rows)
    reach = discount * going
    decay = discount * trace_rate * going

    last = jnp.logical_and(lane == steps - 1, row >= rows - env_rows)
    head_of_row = jnp.broadcast_to(values[:, :1], full)
    after_row = jnp.concatenate([head_of_row[env_rows:], jnp.zeros((env_rows, steps), jnp.float32)], axis=0)
    following = jnp.where(lane == steps - 1, after_row, pltpu.roll(values, steps - 1, 1))
    offset = rewards + reach * following - values
    factor = jnp.where(last, 1.0, decay)

    by = 1
    while by < steps:
        inside = lane < steps - by
        f_next = jnp.where(inside, pltpu.roll(factor, steps - by, 1), 1.0)
        o_next = jnp.where(inside, pltpu.roll(offset, steps - by, 1), 0.0)
        offset = offset + factor * o_next
        factor = factor * f_next
        by *= 2
    f_row = jnp.broadcast_to(factor[:, :1], full)
    o_row = jnp.broadcast_to(offset[:, :1], full)
    f_tail = [jnp.ones((env_rows, steps), jnp.float32)]
    o_tail = [jnp.zeros((env_rows, steps), jnp.float32)]
    for k in range(per_env - 1, 0, -1):
        f_here = f_row[k * env_rows:(k + 1) * env_rows]
        o_here = o_row[k * env_rows:(k + 1) * env_rows]
        o_tail.insert(0, o_here + f_here * o_tail[0])
        f_tail.insert(0, f_here * f_tail[0])
    offset = offset + factor * jnp.concatenate(o_tail, axis=0)
    factor = factor * jnp.concatenate(f_tail, axis=0)

    o_mean, f_mean = mean_of(offset), mean_of(factor)
    o_dev = offset - jnp.concatenate([o_mean] * per_env, axis=0)
    f_dev = factor - jnp.concatenate([f_mean] * per_env, axis=0)
    small = (env_rows, steps)

    def spread(x, at):
        return jnp.broadcast_to(x[:, at:at + 1], small)

    parts = [
        spread(factor[:env_rows], 0),
        spread(offset[:env_rows], 0),
        spread(values[:env_rows], 0),
        spread(reach[rows - env_rows:], steps - 1),
        spread(decay[rows - env_rows:], steps - 1),
        o_mean, f_mean, mean_of(o_dev * o_dev), mean_of(o_dev * f_dev), mean_of(f_dev * f_dev),
    ]
    small_lane = lax.broadcasted_iota(jnp.int32, small, 1)
    message = jnp.zeros(small, jnp.float32)
    for q, part in enumerate(parts):
        message = jnp.where(small_lane == q, part, message)
    tm_buf[0] = message

    pl.semaphore_wait(barrier, n_tm - 1 + n_env - 1)
    copies = [
        pltpu.make_async_remote_copy(
            src_ref=tm_buf.at[0], dst_ref=tm_buf.at[d], send_sem=tm_send.at[d], recv_sem=tm_recv.at[d],
            device_id=(my_env, lax.rem(my_tm + d, n_tm)), device_id_type=MESH,
        )
        for d in range(1, n_tm)
    ]
    for copy in copies:
        copy.start()
    for copy in copies:
        copy.wait()

    next_value = by_env(boot_ref, small, env_rows)
    next_adv = jnp.zeros(small, jnp.float32)
    my_entry = jnp.zeros(small, jnp.float32)
    means, spreads = [], []
    for k in range(n_tm - 1, -1, -1):
        got = tm_buf[lax.rem(my_tm + n_tm - k, n_tm)]
        f0, o0, v0, reach_l, decay_l, om, fm, oo, of, ff = [spread(got, q) for q in range(len(parts))]
        entry = reach_l * next_value + decay_l * next_adv
        my_entry = jnp.where(k == my_tm, entry, my_entry)
        means.append(om + fm * entry)
        spreads.append(oo + (2.0 * of + ff * entry) * entry)
        next_adv = o0 + f0 * entry
        next_value = v0

    def row_mean(x):
        return jnp.broadcast_to(jnp.sum(x, axis=0, keepdims=True) * (1.0 / env_rows), small)

    group_mean = row_mean(sum(means)) * (1.0 / n_tm)
    group_var = row_mean(sum(s + (m - group_mean) * (m - group_mean) for m, s in zip(means, spreads))) * (1.0 / n_tm)
    env_buf[0] = jnp.where(small_lane == 0, group_mean, group_var)
    copies = [
        pltpu.make_async_remote_copy(
            src_ref=env_buf.at[0], dst_ref=env_buf.at[d], send_sem=env_send.at[d], recv_sem=env_recv.at[d],
            device_id=(lax.rem(my_env + d, n_env), my_tm), device_id_type=MESH,
        )
        for d in range(1, n_env)
    ]
    for copy in copies:
        copy.start()
    advantage = offset + factor * jnp.concatenate([my_entry] * per_env, axis=0)
    targets = advantage + values
    for k in range(per_env):
        targets_ref[:, k * steps:(k + 1) * steps] = targets[k * env_rows:(k + 1) * env_rows]
    for copy in copies:
        copy.wait()
    got = [env_buf[lax.rem(my_env + n_env - j, n_env)] for j in range(n_env)]
    env_means = [spread(g, 0) for g in got]
    mean = sum(env_means) * (1.0 / n_env)
    var = sum(spread(g, 1) + (m - mean) * (m - mean) for g, m in zip(got, env_means)) * (1.0 / n_env)
    scale = lax.rsqrt(var + 1e-05)
    for k in range(per_env):
        adv_ref[:, k * steps:(k + 1) * steps] = (advantage[k * env_rows:(k + 1) * env_rows] - mean) * scale


def sweep(n_env, n_tm, dh, th, boot, values, rewards, ends):
    env_rows, local_steps = rewards.shape
    vmem = pl.BlockSpec(memory_space=pltpu.VMEM)
    smem = pl.BlockSpec(memory_space=pltpu.SMEM)
    return pl.pallas_call(
        functools.partial(sweep_kernel, n_env, n_tm),
        out_shape=[jax.ShapeDtypeStruct((env_rows, local_steps), jnp.float32)] * 2,
        in_specs=[smem] * 3 + [vmem] * 3,
        out_specs=[vmem] * 2,
        scratch_shapes=[
            pltpu.VMEM((n_tm, env_rows, BLOCK), jnp.float32),
            pltpu.VMEM((n_env, env_rows, BLOCK), jnp.float32),
            pltpu.SemaphoreType.DMA((n_tm,)),
            pltpu.SemaphoreType.DMA((n_tm,)),
            pltpu.SemaphoreType.DMA((n_env,)),
            pltpu.SemaphoreType.DMA((n_env,)),
        ],
        compiler_params=pltpu.CompilerParams(collective_id=0, has_side_effects=True),
        name="sweep",
    )(dh, th, boot, values, rewards, ends)


def on_device(
    n_env, n_tm, observations, stored_values, rewards, episode_ends, stale_list,
    discount_horizon, trace_horizon, bootstrap, norm_gain, input_weight, value_head,
):
    env_rows, local_steps, features = observations.shape
    slots = env_rows * local_steps // BLOCK
    blocks = observations.reshape(slots, BLOCK, features)
    hidden = input_weight.shape[1]
    values = critic_values(
        stale_list.reshape(slots), blocks, input_weight, stored_values, norm_gain.reshape(1, features),
        value_head.astype(jnp.float32).reshape(hidden // CHUNK, 1, CHUNK),
    )
    return tuple(sweep(
        n_env, n_tm, discount_horizon, trace_horizon, bootstrap, values, rewards, episode_ends
    ))


def solution(mesh):
    in_specs = (
        P("env", "tm", None), P("env", "tm"), P("env", "tm"), P("env", "tm"), P("env", "tm", None),
        P("env"), P("env"), P("env"), P(), P(), P(),
    )
    return jax.shard_map(
        functools.partial(on_device, mesh.shape["env"], mesh.shape["tm"]),
        mesh=mesh, in_specs=in_specs, out_specs=(P("env", "tm"), P("env", "tm")), check_vma=False,
    )
```

```python
import functools

import jax
import jax.numpy as jnp
from jax import lax
from jax.experimental import pallas as pl
from jax.experimental.pallas import tpu as pltpu
from jax.sharding import PartitionSpec as P

BLOCK = 128
CHUNK = 1024
VMEM_MIB = 60
MESH = pl.DeviceIdType.MESH


def partner_of(index):
    return index + 1 - 2 * lax.rem(index, 2)


def share_kernel(list_ref, blocks_ref, their_list_ref, their_blocks_ref, send_sems, recv_sems):
    slots = blocks_ref.shape[0]
    first = slots - their_blocks_ref.shape[0]
    device = (lax.axis_index("env"), partner_of(lax.axis_index("tm")))
    barrier = pltpu.get_barrier_semaphore()
    pl.semaphore_signal(barrier, inc=1, device_id=device, device_id_type=MESH)
    pl.semaphore_wait(barrier, 1)
    copies = [pltpu.make_async_remote_copy(
        src_ref=list_ref, dst_ref=their_list_ref, send_sem=send_sems.at[0], recv_sem=recv_sems.at[0],
        device_id=device, device_id_type=MESH,
    )]
    for i in range(slots - first):
        copies.append(pltpu.make_async_remote_copy(
            src_ref=blocks_ref.at[first + i], dst_ref=their_blocks_ref.at[i],
            send_sem=send_sems.at[1 + i], recv_sem=recv_sems.at[1 + i], device_id=device, device_id_type=MESH,
        ))
    for copy in copies:
        copy.start()
    for copy in copies:
        copy.wait()


def share(listed, blocks, count):
    slots, steps, features = blocks.shape
    hbm = pl.BlockSpec(memory_space=pl.ANY)
    return pl.pallas_call(
        share_kernel,
        out_shape=[
            jax.ShapeDtypeStruct(listed.shape, listed.dtype),
            jax.ShapeDtypeStruct((count, steps, features), blocks.dtype),
        ],
        in_specs=[hbm, hbm],
        out_specs=[hbm, hbm],
        scratch_shapes=[pltpu.SemaphoreType.DMA((count + 1,)), pltpu.SemaphoreType.DMA((count + 1,))],
        compiler_params=pltpu.CompilerParams(
            collective_id=1, has_side_effects=True, vmem_limit_bytes=VMEM_MIB * 1024 * 1024
        ),
        name="share",
    )(listed, blocks)


def critic_kernel(
    list_ref, their_list_ref, blocks_ref, their_blocks_ref, weight_ref, stored_ref, gain_ref, head_ref,
    out_ref, given_ref, back_ref,
    rows_ref, w_ref, head_wide_ref, acc_ref, work_ref, row_sems, w_sems,
):
    slots, steps, features = blocks_ref.shape
    first = slots - their_blocks_ref.shape[0]
    env_rows = stored_ref.shape[0]
    per_env = slots // env_rows
    chunks = head_wide_ref.shape[0]

    def tally(ref):
        stale, movable = jnp.int32(0), jnp.int32(0)
        for i in range(slots):
            stale = stale + jnp.where(ref[i] >= 0, 1, 0).astype(jnp.int32)
            movable = movable + jnp.where(ref[i] >= first, 1, 0).astype(jnp.int32)
        return stale, movable

    mine, mine_movable = tally(list_ref)
    theirs, theirs_movable = tally(their_list_ref)
    give = jnp.minimum(jnp.maximum(mine - theirs, 0) // 2, mine_movable)
    take = jnp.minimum(jnp.maximum(theirs - mine, 0) // 2, theirs_movable)
    count = mine - give + take

    def out_row(number):
        return pl.ds((number % per_env) * env_rows + number // per_env, 1)

    def copy_of(source, i):
        return pltpu.make_async_copy(source, rows_ref.at[pl.ds(i * steps, steps)], row_sems.at[i])

    given_ref[...] = jnp.zeros_like(given_ref)
    back_ref[...] = jnp.zeros_like(back_ref)
    for k in range(per_env):
        out_ref[k * env_rows:(k + 1) * env_rows, :] = stored_ref[:, k * steps:(k + 1) * steps]

    def place(i, state):
        kept, passed = state
        number = list_ref[i]
        goes = jnp.logical_and(number >= first, passed < give)
        stays = jnp.logical_and(number >= 0, jnp.logical_not(goes))

        @pl.when(goes)
        def _():
            given_ref[out_row(number), :] = jnp.ones((1, steps), jnp.float32)

        @pl.when(stays)
        def _():
            work_ref[kept] = number
            copy_of(blocks_ref.at[number], kept).start()

        return kept + stays.astype(jnp.int32), passed + goes.astype(jnp.int32)

    kept, _ = lax.fori_loop(0, slots, place, (jnp.int32(0), jnp.int32(0)))

    def receive(i, taken):
        number = their_list_ref[i]
        comes = jnp.logical_and(number >= first, taken < take)

        @pl.when(comes)
        def _():
            work_ref[kept + taken] = number + slots
            copy_of(their_blocks_ref.at[number - first], kept + taken).start()

        return taken + comes.astype(jnp.int32)

    lax.fori_loop(0, slots, receive, jnp.int32(0))

    def weight_copy(c):
        return pltpu.make_async_copy(
            weight_ref.at[:, pl.ds(pl.multiple_of(c * CHUNK, CHUNK), CHUNK)], w_ref.at[c], w_sems.at[c]
        )

    @pl.when(count > 0)
    def _():
        @pl.loop(0, chunks)
        def _(c):
            weight_copy(c).start()

        for c in range(chunks):
            head_wide_ref[c] = head_ref[:, c * CHUNK:(c + 1) * CHUNK].astype(jnp.float32)
        acc_ref[...] = jnp.zeros_like(acc_ref)

        @pl.loop(0, count)
        def _(i):
            copy_of(blocks_ref.at[0], i).wait()
            here = pl.ds(pl.multiple_of(i * steps, steps), steps)
            wide = rows_ref[here, :].astype(jnp.float32)
            mean = jnp.sum(wide * wide, axis=-1, keepdims=True) * (1.0 / features)
            rows_ref[here, :] = (wide * lax.rsqrt(mean + 1e-05) * gain_ref[...]).astype(jnp.bfloat16)

        def tile(c, start, size):
            here = pl.ds(pl.multiple_of(start, steps), size)
            hidden = jnp.dot(rows_ref[here, :], w_ref[c], preferred_element_type=jnp.float32)
            half = 0.5 * hidden
            active = (half + half * jnp.tanh(half)).astype(jnp.bfloat16).astype(jnp.float32)
            part = active * head_wide_ref[c]
            total = part[:, :128]
            for j in range(1, CHUNK // 128):
                total = total + part[:, j * 128:(j + 1) * 128]
            acc_ref[here, :] += total

        @pl.loop(0, chunks)
        def _(c):
            weight_copy(c).wait()

            @pl.loop(0, count // 8)
            def _(q):
                tile(c, q * (8 * steps), 8 * steps)

            for size in (4, 2, 1):
                @pl.when((count // size) % 2 == 1)
                def _(size=size):
                    tile(c, (count // (2 * size)) * (2 * size * steps), size * steps)

        @pl.loop(0, count)
        def _(i):
            here = pl.ds(pl.multiple_of(i * steps, steps), steps)
            score = jnp.sum(acc_ref[here, :].T, axis=0, keepdims=True)
            number = work_ref[i]

            @pl.when(number < slots)
            def _():
                out_ref[out_row(number), :] = score

            @pl.when(number >= slots)
            def _():
                back_ref[out_row(number - slots), :] = score


def critic_values(listed, blocks, weight, stored, gain, head):
    slots, steps, features = blocks.shape
    chunks = weight.shape[1] // CHUNK
    their_list, their_blocks = share(listed, blocks, slots // 2)
    vmem = pl.BlockSpec(memory_space=pltpu.VMEM)
    smem = pl.BlockSpec(memory_space=pltpu.SMEM)
    hbm = pl.BlockSpec(memory_space=pl.ANY)
    return pl.pallas_call(
        critic_kernel,
        out_shape=[jax.ShapeDtypeStruct((slots, steps), jnp.float32)] * 3,
        in_specs=[smem, smem, hbm, hbm, hbm, vmem, vmem, vmem],
        out_specs=[vmem] * 3,
        scratch_shapes=[
            pltpu.VMEM((slots * steps, features), jnp.bfloat16),
            pltpu.VMEM((chunks, features, CHUNK), jnp.bfloat16),
            pltpu.VMEM((chunks, 1, CHUNK), jnp.float32),
            pltpu.VMEM((slots * steps, 128), jnp.float32),
            pltpu.SMEM((slots,), jnp.int32),
            pltpu.SemaphoreType.DMA((slots,)),
            pltpu.SemaphoreType.DMA((chunks,)),
        ],
        compiler_params=pltpu.CompilerParams(vmem_limit_bytes=VMEM_MIB * 1024 * 1024),
        name="critic",
    )(listed, their_list, blocks, their_blocks, weight, stored, gain, head)


def sweep_kernel(
    n_env, n_tm, dh_ref, th_ref, boot_ref, values_ref, given_ref, back_ref, rewards_ref, ends_ref,
    targets_ref, adv_ref, scored_buf, tm_buf, env_buf, scored_send, scored_recv, tm_send, tm_recv, env_send, env_recv,
):
    env_rows, local_steps = rewards_ref.shape
    rows, steps = values_ref.shape
    per_env = rows // env_rows
    my_env, my_tm = lax.axis_index("env"), lax.axis_index("tm")

    barrier = pltpu.get_barrier_semaphore()
    for d in range(1, n_tm):
        pl.semaphore_signal(barrier, inc=1, device_id=(my_env, lax.rem(my_tm + d, n_tm)), device_id_type=MESH)
    for d in range(1, n_env):
        pl.semaphore_signal(barrier, inc=1, device_id=(lax.rem(my_env + d, n_env), my_tm), device_id_type=MESH)

    def stacked(ref):
        return jnp.concatenate([ref[:, k * steps:(k + 1) * steps] for k in range(per_env)], axis=0)

    def by_env(ref, shape, modulus):
        env_of = lax.broadcasted_iota(jnp.int32, shape, 0) % modulus
        out = jnp.full(shape, ref[0], jnp.float32)
        for e in range(1, env_rows):
            out = jnp.where(env_of == e, ref[e], out)
        return out

    def over_blocks(x):
        total = x[:env_rows]
        for k in range(1, per_env):
            total = total + x[k * env_rows:(k + 1) * env_rows]
        return total

    def mean_of(x):
        total = jnp.sum(over_blocks(x), axis=1, keepdims=True) * (1.0 / local_steps)
        return jnp.broadcast_to(total, (env_rows, steps))

    full = (rows, steps)
    lane = lax.broadcasted_iota(jnp.int32, full, 1)
    row = lax.broadcasted_iota(jnp.int32, full, 0)
    pl.semaphore_wait(barrier, n_tm - 1 + n_env - 1)
    scored = pltpu.make_async_remote_copy(
        src_ref=back_ref, dst_ref=scored_buf, send_sem=scored_send, recv_sem=scored_recv,
        device_id=(my_env, partner_of(my_tm)), device_id_type=MESH,
    )
    scored.start()
    rewards = stacked(rewards_ref)
    going = 1.0 - stacked(ends_ref).astype(jnp.float32)
    discount = 1.0 - 1.0 / by_env(dh_ref, full, env_rows)
    trace_rate = 1.0 - 1.0 / by_env(th_ref, full, env_rows)
    reach = discount * going
    decay = discount * trace_rate * going

    scored.wait()
    values = jnp.where(given_ref[...] > 0.5, scored_buf[...], values_ref[...])

    last = jnp.logical_and(lane == steps - 1, row >= rows - env_rows)
    head_of_row = jnp.broadcast_to(values[:, :1], full)
    after_row = jnp.concatenate([head_of_row[env_rows:], jnp.zeros((env_rows, steps), jnp.float32)], axis=0)
    following = jnp.where(lane == steps - 1, after_row, pltpu.roll(values, steps - 1, 1))
    offset = rewards + reach * following - values
    factor = jnp.where(last, 1.0, decay)

    by = 1
    while by < steps:
        inside = lane < steps - by
        f_next = jnp.where(inside, pltpu.roll(factor, steps - by, 1), 1.0)
        o_next = jnp.where(inside, pltpu.roll(offset, steps - by, 1), 0.0)
        offset = offset + factor * o_next
        factor = factor * f_next
        by *= 2
    f_row = jnp.broadcast_to(factor[:, :1], full)
    o_row = jnp.broadcast_to(offset[:, :1], full)
    f_tail = [jnp.ones((env_rows, steps), jnp.float32)]
    o_tail = [jnp.zeros((env_rows, steps), jnp.float32)]
    for k in range(per_env - 1, 0, -1):
        f_here = f_row[k * env_rows:(k + 1) * env_rows]
        o_here = o_row[k * env_rows:(k + 1) * env_rows]
        o_tail.insert(0, o_here + f_here * o_tail[0])
        f_tail.insert(0, f_here * f_tail[0])
    offset = offset + factor * jnp.concatenate(o_tail, axis=0)
    factor = factor * jnp.concatenate(f_tail, axis=0)

    o_mean, f_mean = mean_of(offset), mean_of(factor)
    o_dev = offset - jnp.concatenate([o_mean] * per_env, axis=0)
    f_dev = factor - jnp.concatenate([f_mean] * per_env, axis=0)
    small = (env_rows, steps)

    def spread(x, at):
        return jnp.broadcast_to(x[:, at:at + 1], small)

    parts = [
        spread(factor[:env_rows], 0),
        spread(offset[:env_rows], 0),
        spread(values[:env_rows], 0),
        spread(reach[rows - env_rows:], steps - 1),
        spread(decay[rows - env_rows:], steps - 1),
        o_mean, f_mean, mean_of(o_dev * o_dev), mean_of(o_dev * f_dev), mean_of(f_dev * f_dev),
    ]
    small_lane = lax.broadcasted_iota(jnp.int32, small, 1)
    message = jnp.zeros(small, jnp.float32)
    for q, part in enumerate(parts):
        message = jnp.where(small_lane == q, part, message)
    tm_buf[0] = message

    copies = [
        pltpu.make_async_remote_copy(
            src_ref=tm_buf.at[0], dst_ref=tm_buf.at[d], send_sem=tm_send.at[d], recv_sem=tm_recv.at[d],
            device_id=(my_env, lax.rem(my_tm + d, n_tm)), device_id_type=MESH,
        )
        for d in range(1, n_tm)
    ]
    for copy in copies:
        copy.start()
    for copy in copies:
        copy.wait()

    next_value = by_env(boot_ref, small, env_rows)
    next_adv = jnp.zeros(small, jnp.float32)
    my_entry = jnp.zeros(small, jnp.float32)
    means, spreads = [], []
    for k in range(n_tm - 1, -1, -1):
        got = tm_buf[lax.rem(my_tm + n_tm - k, n_tm)]
        f0, o0, v0, reach_l, decay_l, om, fm, oo, of, ff = [spread(got, q) for q in range(len(parts))]
        entry = reach_l * next_value + decay_l * next_adv
        my_entry = jnp.where(k == my_tm, entry, my_entry)
        means.append(om + fm * entry)
        spreads.append(oo + (2.0 * of + ff * entry) * entry)
        next_adv = o0 + f0 * entry
        next_value = v0

    def row_mean(x):
        return jnp.broadcast_to(jnp.sum(x, axis=0, keepdims=True) * (1.0 / env_rows), small)

    group_mean = row_mean(sum(means)) * (1.0 / n_tm)
    group_var = row_mean(sum(s + (m - group_mean) * (m - group_mean) for m, s in zip(means, spreads))) * (1.0 / n_tm)
    env_buf[0] = jnp.where(small_lane == 0, group_mean, group_var)
    copies = [
        pltpu.make_async_remote_copy(
            src_ref=env_buf.at[0], dst_ref=env_buf.at[d], send_sem=env_send.at[d], recv_sem=env_recv.at[d],
            device_id=(lax.rem(my_env + d, n_env), my_tm), device_id_type=MESH,
        )
        for d in range(1, n_env)
    ]
    for copy in copies:
        copy.start()
    advantage = offset + factor * jnp.concatenate([my_entry] * per_env, axis=0)
    targets = advantage + values
    for k in range(per_env):
        targets_ref[:, k * steps:(k + 1) * steps] = targets[k * env_rows:(k + 1) * env_rows]
    for copy in copies:
        copy.wait()
    got = [env_buf[lax.rem(my_env + n_env - j, n_env)] for j in range(n_env)]
    env_means = [spread(g, 0) for g in got]
    mean = sum(env_means) * (1.0 / n_env)
    var = sum(spread(g, 1) + (m - mean) * (m - mean) for g, m in zip(got, env_means)) * (1.0 / n_env)
    scale = lax.rsqrt(var + 1e-05)
    for k in range(per_env):
        adv_ref[:, k * steps:(k + 1) * steps] = (advantage[k * env_rows:(k + 1) * env_rows] - mean) * scale


def sweep(n_env, n_tm, dh, th, boot, values, given, back, rewards, ends):
    env_rows, local_steps = rewards.shape
    vmem = pl.BlockSpec(memory_space=pltpu.VMEM)
    smem = pl.BlockSpec(memory_space=pltpu.SMEM)
    return pl.pallas_call(
        functools.partial(sweep_kernel, n_env, n_tm),
        out_shape=[jax.ShapeDtypeStruct((env_rows, local_steps), jnp.float32)] * 2,
        in_specs=[smem] * 3 + [vmem] * 5,
        out_specs=[vmem] * 2,
        scratch_shapes=[
            pltpu.VMEM(values.shape, jnp.float32),
            pltpu.VMEM((n_tm, env_rows, BLOCK), jnp.float32),
            pltpu.VMEM((n_env, env_rows, BLOCK), jnp.float32),
            pltpu.SemaphoreType.DMA,
            pltpu.SemaphoreType.DMA,
            pltpu.SemaphoreType.DMA((n_tm,)),
            pltpu.SemaphoreType.DMA((n_tm,)),
            pltpu.SemaphoreType.DMA((n_env,)),
            pltpu.SemaphoreType.DMA((n_env,)),
        ],
        compiler_params=pltpu.CompilerParams(
            collective_id=0, has_side_effects=True, vmem_limit_bytes=VMEM_MIB * 1024 * 1024
        ),
        name="sweep",
    )(dh, th, boot, values, given, back, rewards, ends)


def on_device(
    n_env, n_tm, observations, stored_values, rewards, episode_ends, stale_list,
    discount_horizon, trace_horizon, bootstrap, norm_gain, input_weight, value_head,
):
    env_rows, local_steps, features = observations.shape
    slots = env_rows * local_steps // BLOCK
    blocks = observations.reshape(slots, BLOCK, features)
    hidden = input_weight.shape[1]
    values, given, back = critic_values(
        stale_list.reshape(slots), blocks, input_weight, stored_values, norm_gain.reshape(1, features),
        value_head.reshape(1, hidden),
    )
    return tuple(sweep(
        n_env, n_tm, discount_horizon, trace_horizon, bootstrap, values, given, back, rewards, episode_ends
    ))


def solution(mesh):
    in_specs = (
        P("env", "tm", None), P("env", "tm"), P("env", "tm"), P("env", "tm"), P("env", "tm", None),
        P("env"), P("env"), P("env"), P(), P(), P(),
    )
    return jax.shard_map(
        functools.partial(on_device, mesh.shape["env"], mesh.shape["tm"]),
        mesh=mesh, in_specs=in_specs, out_specs=(P("env", "tm"), P("env", "tm")), check_vma=False,
    )
```

```python
import functools

import jax
import jax.numpy as jnp
from jax import lax
from jax.experimental import pallas as pl
from jax.experimental.pallas import tpu as pltpu
from jax.sharding import PartitionSpec as P

BLOCK = 128
CHUNK = 1024
VMEM_MIB = 60
MESH = pl.DeviceIdType.MESH


def partner_of(index):
    return index + 1 - 2 * lax.rem(index, 2)


def share_kernel(list_ref, blocks_ref, their_list_ref, their_blocks_ref, send_sems, recv_sems):
    slots = blocks_ref.shape[0]
    first = slots - their_blocks_ref.shape[0]
    device = (lax.axis_index("env"), partner_of(lax.axis_index("tm")))
    barrier = pltpu.get_barrier_semaphore()
    pl.semaphore_signal(barrier, inc=1, device_id=device, device_id_type=MESH)
    pl.semaphore_wait(barrier, 1)
    copies = [pltpu.make_async_remote_copy(
        src_ref=list_ref, dst_ref=their_list_ref, send_sem=send_sems.at[0], recv_sem=recv_sems.at[0],
        device_id=device, device_id_type=MESH,
    )]
    for i in range(slots - first):
        copies.append(pltpu.make_async_remote_copy(
            src_ref=blocks_ref.at[first + i], dst_ref=their_blocks_ref.at[i],
            send_sem=send_sems.at[1 + i], recv_sem=recv_sems.at[1 + i], device_id=device, device_id_type=MESH,
        ))
    for copy in copies:
        copy.start()
    for copy in copies:
        copy.wait()


def share(listed, blocks, count):
    slots, steps, features = blocks.shape
    hbm = pl.BlockSpec(memory_space=pl.ANY)
    return pl.pallas_call(
        share_kernel,
        out_shape=[
            jax.ShapeDtypeStruct(listed.shape, listed.dtype),
            jax.ShapeDtypeStruct((count, steps, features), blocks.dtype),
        ],
        in_specs=[hbm, hbm],
        out_specs=[hbm, hbm],
        scratch_shapes=[pltpu.SemaphoreType.DMA((count + 1,)), pltpu.SemaphoreType.DMA((count + 1,))],
        compiler_params=pltpu.CompilerParams(
            collective_id=1, has_side_effects=True, vmem_limit_bytes=VMEM_MIB * 1024 * 1024
        ),
        name="share",
    )(listed, blocks)


def critic_kernel(
    list_ref, their_list_ref, blocks_ref, their_blocks_ref, weight_ref, stored_ref, gain_ref, head_ref,
    out_ref, given_ref, back_ref,
    rows_ref, w_ref, head_wide_ref, acc_ref, work_ref, row_sems, w_sems,
):
    slots, steps, features = blocks_ref.shape
    first = slots - their_blocks_ref.shape[0]
    env_rows = stored_ref.shape[0]
    per_env = slots // env_rows
    chunks = head_wide_ref.shape[0]

    def tally(ref):
        stale, movable = jnp.int32(0), jnp.int32(0)
        for i in range(slots):
            stale = stale + jnp.where(ref[i] >= 0, 1, 0).astype(jnp.int32)
            movable = movable + jnp.where(ref[i] >= first, 1, 0).astype(jnp.int32)
        return stale, movable

    mine, mine_movable = tally(list_ref)
    theirs, theirs_movable = tally(their_list_ref)
    give = jnp.minimum(jnp.maximum(mine - theirs, 0) // 2, mine_movable)
    take = jnp.minimum(jnp.maximum(theirs - mine, 0) // 2, theirs_movable)
    count = mine - give + take

    def out_row(number):
        return pl.ds((number % per_env) * env_rows + number // per_env, 1)

    def copy_of(source, i):
        return pltpu.make_async_copy(source, rows_ref.at[pl.ds(i * steps, steps)], row_sems.at[i])

    given_ref[...] = jnp.zeros_like(given_ref)
    back_ref[...] = jnp.zeros_like(back_ref)
    for k in range(per_env):
        out_ref[k * env_rows:(k + 1) * env_rows, :] = stored_ref[:, k * steps:(k + 1) * steps]

    def place(i, state):
        kept, passed = state
        number = list_ref[i]
        goes = jnp.logical_and(number >= first, passed < give)
        stays = jnp.logical_and(number >= 0, jnp.logical_not(goes))

        @pl.when(goes)
        def _():
            given_ref[out_row(number), :] = jnp.ones((1, steps), jnp.float32)

        @pl.when(stays)
        def _():
            work_ref[kept] = number
            copy_of(blocks_ref.at[number], kept).start()

        return kept + stays.astype(jnp.int32), passed + goes.astype(jnp.int32)

    kept, _ = lax.fori_loop(0, slots, place, (jnp.int32(0), jnp.int32(0)))

    def receive(i, taken):
        number = their_list_ref[i]
        comes = jnp.logical_and(number >= first, taken < take)

        @pl.when(comes)
        def _():
            work_ref[kept + taken] = number + slots
            copy_of(their_blocks_ref.at[number - first], kept + taken).start()

        return taken + comes.astype(jnp.int32)

    lax.fori_loop(0, slots, receive, jnp.int32(0))

    def weight_copy(c):
        return pltpu.make_async_copy(
            weight_ref.at[:, pl.ds(pl.multiple_of(c * CHUNK, CHUNK), CHUNK)], w_ref.at[c], w_sems.at[c]
        )

    @pl.when(count > 0)
    def _():
        @pl.loop(0, chunks)
        def _(c):
            weight_copy(c).start()

        for c in range(chunks):
            head_wide_ref[c] = head_ref[:, c * CHUNK:(c + 1) * CHUNK].astype(jnp.float32)
        acc_ref[...] = jnp.zeros_like(acc_ref)

        @pl.loop(0, count)
        def _(i):
            copy_of(blocks_ref.at[0], i).wait()
            here = pl.ds(pl.multiple_of(i * steps, steps), steps)
            wide = rows_ref[here, :].astype(jnp.float32)
            mean = jnp.sum(wide * wide, axis=-1, keepdims=True) * (1.0 / features)
            rows_ref[here, :] = (wide * lax.rsqrt(mean + 1e-05) * gain_ref[...]).astype(jnp.bfloat16)

        def tile(c, start, size):
            here = pl.ds(pl.multiple_of(start, steps), size)
            hidden = jnp.dot(rows_ref[here, :], w_ref[c], preferred_element_type=jnp.float32)
            half = 0.5 * hidden
            active = (half + half * jnp.tanh(half)).astype(jnp.bfloat16).astype(jnp.float32)
            part = active * head_wide_ref[c]
            total = part[:, :128]
            for j in range(1, CHUNK // 128):
                total = total + part[:, j * 128:(j + 1) * 128]
            acc_ref[here, :] += total

        @pl.loop(0, chunks)
        def _(c):
            weight_copy(c).wait()

            @pl.loop(0, count // 8)
            def _(q):
                tile(c, q * (8 * steps), 8 * steps)

            for size in (4, 2, 1):
                @pl.when((count // size) % 2 == 1)
                def _(size=size):
                    tile(c, (count // (2 * size)) * (2 * size * steps), size * steps)

        @pl.loop(0, count)
        def _(i):
            here = pl.ds(pl.multiple_of(i * steps, steps), steps)
            score = jnp.sum(acc_ref[here, :].T, axis=0, keepdims=True)
            number = work_ref[i]

            @pl.when(number < slots)
            def _():
                out_ref[out_row(number), :] = score

            @pl.when(number >= slots)
            def _():
                back_ref[out_row(number - slots), :] = score


def critic_values(listed, blocks, weight, stored, gain, head):
    slots, steps, features = blocks.shape
    chunks = weight.shape[1] // CHUNK
    their_list, their_blocks = share(listed, blocks, slots // 3)
    vmem = pl.BlockSpec(memory_space=pltpu.VMEM)
    smem = pl.BlockSpec(memory_space=pltpu.SMEM)
    hbm = pl.BlockSpec(memory_space=pl.ANY)
    return pl.pallas_call(
        critic_kernel,
        out_shape=[jax.ShapeDtypeStruct((slots, steps), jnp.float32)] * 3,
        in_specs=[smem, smem, hbm, hbm, hbm, vmem, vmem, vmem],
        out_specs=[vmem] * 3,
        scratch_shapes=[
            pltpu.VMEM((slots * steps, features), jnp.bfloat16),
            pltpu.VMEM((chunks, features, CHUNK), jnp.bfloat16),
            pltpu.VMEM((chunks, 1, CHUNK), jnp.float32),
            pltpu.VMEM((slots * steps, 128), jnp.float32),
            pltpu.SMEM((slots,), jnp.int32),
            pltpu.SemaphoreType.DMA((slots,)),
            pltpu.SemaphoreType.DMA((chunks,)),
        ],
        compiler_params=pltpu.CompilerParams(vmem_limit_bytes=VMEM_MIB * 1024 * 1024),
        name="critic",
    )(listed, their_list, blocks, their_blocks, weight, stored, gain, head)


def sweep_kernel(
    n_env, n_tm, dh_ref, th_ref, boot_ref, values_ref, given_ref, back_ref, rewards_ref, ends_ref,
    targets_ref, adv_ref, scored_buf, tm_buf, env_buf, scored_send, scored_recv, tm_send, tm_recv, env_send, env_recv,
):
    env_rows, local_steps = rewards_ref.shape
    rows, steps = values_ref.shape
    per_env = rows // env_rows
    my_env, my_tm = lax.axis_index("env"), lax.axis_index("tm")

    barrier = pltpu.get_barrier_semaphore()
    for d in range(1, n_tm):
        pl.semaphore_signal(barrier, inc=1, device_id=(my_env, lax.rem(my_tm + d, n_tm)), device_id_type=MESH)
    for d in range(1, n_env):
        pl.semaphore_signal(barrier, inc=1, device_id=(lax.rem(my_env + d, n_env), my_tm), device_id_type=MESH)

    def stacked(ref):
        return jnp.concatenate([ref[:, k * steps:(k + 1) * steps] for k in range(per_env)], axis=0)

    def by_env(ref, shape, modulus):
        env_of = lax.broadcasted_iota(jnp.int32, shape, 0) % modulus
        out = jnp.full(shape, ref[0], jnp.float32)
        for e in range(1, env_rows):
            out = jnp.where(env_of == e, ref[e], out)
        return out

    def over_blocks(x):
        total = x[:env_rows]
        for k in range(1, per_env):
            total = total + x[k * env_rows:(k + 1) * env_rows]
        return total

    def mean_of(x):
        total = jnp.sum(over_blocks(x), axis=1, keepdims=True) * (1.0 / local_steps)
        return jnp.broadcast_to(total, (env_rows, steps))

    full = (rows, steps)
    lane = lax.broadcasted_iota(jnp.int32, full, 1)
    row = lax.broadcasted_iota(jnp.int32, full, 0)
    pl.semaphore_wait(barrier, n_tm - 1 + n_env - 1)
    scored = pltpu.make_async_remote_copy(
        src_ref=back_ref, dst_ref=scored_buf, send_sem=scored_send, recv_sem=scored_recv,
        device_id=(my_env, partner_of(my_tm)), device_id_type=MESH,
    )
    scored.start()
    rewards = stacked(rewards_ref)
    going = 1.0 - stacked(ends_ref).astype(jnp.float32)
    discount = 1.0 - 1.0 / by_env(dh_ref, full, env_rows)
    trace_rate = 1.0 - 1.0 / by_env(th_ref, full, env_rows)
    reach = discount * going
    decay = discount * trace_rate * going

    scored.wait()
    values = jnp.where(given_ref[...] > 0.5, scored_buf[...], values_ref[...])

    last = jnp.logical_and(lane == steps - 1, row >= rows - env_rows)
    head_of_row = jnp.broadcast_to(values[:, :1], full)
    after_row = jnp.concatenate([head_of_row[env_rows:], jnp.zeros((env_rows, steps), jnp.float32)], axis=0)
    following = jnp.where(lane == steps - 1, after_row, pltpu.roll(values, steps - 1, 1))
    offset = rewards + reach * following - values
    factor = jnp.where(last, 1.0, decay)

    by = 1
    while by < steps:
        inside = lane < steps - by
        f_next = jnp.where(inside, pltpu.roll(factor, steps - by, 1), 1.0)
        o_next = jnp.where(inside, pltpu.roll(offset, steps - by, 1), 0.0)
        offset = offset + factor * o_next
        factor = factor * f_next
        by *= 2
    f_row = jnp.broadcast_to(factor[:, :1], full)
    o_row = jnp.broadcast_to(offset[:, :1], full)
    f_tail = [jnp.ones((env_rows, steps), jnp.float32)]
    o_tail = [jnp.zeros((env_rows, steps), jnp.float32)]
    for k in range(per_env - 1, 0, -1):
        f_here = f_row[k * env_rows:(k + 1) * env_rows]
        o_here = o_row[k * env_rows:(k + 1) * env_rows]
        o_tail.insert(0, o_here + f_here * o_tail[0])
        f_tail.insert(0, f_here * f_tail[0])
    offset = offset + factor * jnp.concatenate(o_tail, axis=0)
    factor = factor * jnp.concatenate(f_tail, axis=0)

    o_mean, f_mean = mean_of(offset), mean_of(factor)
    o_dev = offset - jnp.concatenate([o_mean] * per_env, axis=0)
    f_dev = factor - jnp.concatenate([f_mean] * per_env, axis=0)
    small = (env_rows, steps)

    def spread(x, at):
        return jnp.broadcast_to(x[:, at:at + 1], small)

    parts = [
        spread(factor[:env_rows], 0),
        spread(offset[:env_rows], 0),
        spread(values[:env_rows], 0),
        spread(reach[rows - env_rows:], steps - 1),
        spread(decay[rows - env_rows:], steps - 1),
        o_mean, f_mean, mean_of(o_dev * o_dev), mean_of(o_dev * f_dev), mean_of(f_dev * f_dev),
    ]
    small_lane = lax.broadcasted_iota(jnp.int32, small, 1)
    message = jnp.zeros(small, jnp.float32)
    for q, part in enumerate(parts):
        message = jnp.where(small_lane == q, part, message)
    tm_buf[0] = message

    copies = [
        pltpu.make_async_remote_copy(
            src_ref=tm_buf.at[0], dst_ref=tm_buf.at[d], send_sem=tm_send.at[d], recv_sem=tm_recv.at[d],
            device_id=(my_env, lax.rem(my_tm + d, n_tm)), device_id_type=MESH,
        )
        for d in range(1, n_tm)
    ]
    for copy in copies:
        copy.start()
    for copy in copies:
        copy.wait()

    next_value = by_env(boot_ref, small, env_rows)
    next_adv = jnp.zeros(small, jnp.float32)
    my_entry = jnp.zeros(small, jnp.float32)
    means, spreads = [], []
    for k in range(n_tm - 1, -1, -1):
        got = tm_buf[lax.rem(my_tm + n_tm - k, n_tm)]
        f0, o0, v0, reach_l, decay_l, om, fm, oo, of, ff = [spread(got, q) for q in range(len(parts))]
        entry = reach_l * next_value + decay_l * next_adv
        my_entry = jnp.where(k == my_tm, entry, my_entry)
        means.append(om + fm * entry)
        spreads.append(oo + (2.0 * of + ff * entry) * entry)
        next_adv = o0 + f0 * entry
        next_value = v0

    def row_mean(x):
        return jnp.broadcast_to(jnp.sum(x, axis=0, keepdims=True) * (1.0 / env_rows), small)

    group_mean = row_mean(sum(means)) * (1.0 / n_tm)
    group_var = row_mean(sum(s + (m - group_mean) * (m - group_mean) for m, s in zip(means, spreads))) * (1.0 / n_tm)
    env_buf[0] = jnp.where(small_lane == 0, group_mean, group_var)
    copies = [
        pltpu.make_async_remote_copy(
            src_ref=env_buf.at[0], dst_ref=env_buf.at[d], send_sem=env_send.at[d], recv_sem=env_recv.at[d],
            device_id=(lax.rem(my_env + d, n_env), my_tm), device_id_type=MESH,
        )
        for d in range(1, n_env)
    ]
    for copy in copies:
        copy.start()
    advantage = offset + factor * jnp.concatenate([my_entry] * per_env, axis=0)
    targets = advantage + values
    for k in range(per_env):
        targets_ref[:, k * steps:(k + 1) * steps] = targets[k * env_rows:(k + 1) * env_rows]
    for copy in copies:
        copy.wait()
    got = [env_buf[lax.rem(my_env + n_env - j, n_env)] for j in range(n_env)]
    env_means = [spread(g, 0) for g in got]
    mean = sum(env_means) * (1.0 / n_env)
    var = sum(spread(g, 1) + (m - mean) * (m - mean) for g, m in zip(got, env_means)) * (1.0 / n_env)
    scale = lax.rsqrt(var + 1e-05)
    for k in range(per_env):
        adv_ref[:, k * steps:(k + 1) * steps] = (advantage[k * env_rows:(k + 1) * env_rows] - mean) * scale


def sweep(n_env, n_tm, dh, th, boot, values, given, back, rewards, ends):
    env_rows, local_steps = rewards.shape
    vmem = pl.BlockSpec(memory_space=pltpu.VMEM)
    smem = pl.BlockSpec(memory_space=pltpu.SMEM)
    return pl.pallas_call(
        functools.partial(sweep_kernel, n_env, n_tm),
        out_shape=[jax.ShapeDtypeStruct((env_rows, local_steps), jnp.float32)] * 2,
        in_specs=[smem] * 3 + [vmem] * 5,
        out_specs=[vmem] * 2,
        scratch_shapes=[
            pltpu.VMEM(values.shape, jnp.float32),
            pltpu.VMEM((n_tm, env_rows, BLOCK), jnp.float32),
            pltpu.VMEM((n_env, env_rows, BLOCK), jnp.float32),
            pltpu.SemaphoreType.DMA,
            pltpu.SemaphoreType.DMA,
            pltpu.SemaphoreType.DMA((n_tm,)),
            pltpu.SemaphoreType.DMA((n_tm,)),
            pltpu.SemaphoreType.DMA((n_env,)),
            pltpu.SemaphoreType.DMA((n_env,)),
        ],
        compiler_params=pltpu.CompilerParams(
            collective_id=0, has_side_effects=True, vmem_limit_bytes=VMEM_MIB * 1024 * 1024
        ),
        name="sweep",
    )(dh, th, boot, values, given, back, rewards, ends)


def on_device(
    n_env, n_tm, observations, stored_values, rewards, episode_ends, stale_list,
    discount_horizon, trace_horizon, bootstrap, norm_gain, input_weight, value_head,
):
    env_rows, local_steps, features = observations.shape
    slots = env_rows * local_steps // BLOCK
    blocks = observations.reshape(slots, BLOCK, features)
    hidden = input_weight.shape[1]
    values, given, back = critic_values(
        stale_list.reshape(slots), blocks, input_weight, stored_values, norm_gain.reshape(1, features),
        value_head.reshape(1, hidden),
    )
    return tuple(sweep(
        n_env, n_tm, discount_horizon, trace_horizon, bootstrap, values, given, back, rewards, episode_ends
    ))


def solution(mesh):
    in_specs = (
        P("env", "tm", None), P("env", "tm"), P("env", "tm"), P("env", "tm"), P("env", "tm", None),
        P("env"), P("env"), P("env"), P(), P(), P(),
    )
    return jax.shard_map(
        functools.partial(on_device, mesh.shape["env"], mesh.shape["tm"]),
        mesh=mesh, in_specs=in_specs, out_specs=(P("env", "tm"), P("env", "tm")), check_vma=False,
    )
```
